32 devices in a mesh: grp: 4 (over y, core), rows: 8 (over z, x).
Axes of the slice: x: 2, y: 2, z: 4, core: 2. Of those that a mesh axis runs over, the one named last changes fastest.
Arguments:
- rhs: float32 [2048, 64, 128], P(('grp', 'rows')), may hold values from -6 to 6
- fine_diag: bfloat16 [2048, 64, 64], P(('grp', 'rows')), may hold values from -0.2 to 1.2
- fine_smoother: bfloat16 [2048, 64, 64], P(('grp', 'rows')), may hold values from -4 to 4
- fine_blocks: bfloat16 [2048, 7, 64, 64], P(('grp', 'rows')), may hold values from -0.1796875 to 0.1796875
- fine_cols: int32 [2048, 7], P(('grp', 'rows')), may hold values from 0 to 2047, as said below
- aggregate: int32 [2048], P(('grp', 'rows')), may hold values from 0 to 511, as said below
- coarse_diag: bfloat16 [512, 64, 64], P('rows'), may hold values from -0.8 to 4.8
- coarse_smoother: bfloat16 [512, 64, 64], P('rows'), may hold values from -1 to 1
- coarse_blocks: bfloat16 [512, 7, 64, 64], P('rows'), may hold values from -0.71875 to 0.71875
- coarse_cols: int32 [512, 7], P('rows'), may hold values from 0 to 511, as said below
Outputs:
- solution: float32 [2048, 64, 128], P(('grp', 'rows'))
The draws below stay inside these ranges and needn't reach their ends.
Inputs may be any that keep to these rules, and one draw needn't show every extreme that they name: fine_cols row i names rows within 32 of i; the distance 32 is reached. coarse_cols row c names rows within 32 of c; the distance 32 is reached. `aggregate`: aggregate_i lies in [r * 64, (r + 1) * 64) with r = (i // 64) mod 8.
All inputs are finite; a program needn't handle non-finite values.
Results may differ from the reference program's by a relative error of at most 0.001.
The reference program's roundings to bfloat16 on the way count: a program that leaves them out, or rounds other values in their place, can miss the bound.
Values may be sent and summed in bfloat16 or wider, within the bound.
A program may use at most 128 MiB of HBM per device.

```python
import jax
import jax.numpy as jnp
from jax import lax

B = 64
NEIGH = 7
R_DEV = 64
NRHS = 128
C_DEV = 64
NF = 2048
NC = 512
N_ROWS = 8


def build_blocks(key, count, scale):
    shape = (count, B, B)
    noise = jnp.clip(0.04 * jax.random.normal(key, shape, jnp.float32), -0.16, 0.16)
    return scale * (jnp.eye(B, dtype=jnp.float32)[None] + noise)


def neighbour_columns(key, count, reach, block):
    key_distance, key_direction, key_chosen = jax.random.split(key, 3)
    distance = jax.random.randint(key_distance, (count, NEIGH), 1, reach + 1)
    direction = 2 * jax.random.randint(key_direction, (count, NEIGH), 0, 2) - 1
    offset = distance * direction
    row_ids = jnp.arange(count, dtype=jnp.int32)
    groups = count // block
    chosen = jax.random.randint(key_chosen, (groups, 2), 0, block)
    within = row_ids % block
    owner_block = row_ids // block
    low_hit = within == chosen[owner_block, 0]
    high_hit = within == chosen[owner_block, 1]
    first_slot = jnp.where(high_hit, reach, jnp.where(low_hit, -reach, offset[:, 0]))
    second_slot = jnp.where(row_ids == 0, -reach, jnp.where(row_ids == count - 1, reach, offset[:, 1]))
    offset = jnp.concatenate([first_slot[:, None], second_slot[:, None], offset[:, 2:]], axis=1)
    return jnp.clip(row_ids[:, None] + offset, 0, count - 1).astype(jnp.int32)


def draw_fine_diag(key, part):
    return build_blocks(jax.random.fold_in(key, 11), NF, 1.0).astype(jnp.bfloat16)


def draw_fine_smoother(key, part):
    return jnp.linalg.inv(build_blocks(jax.random.fold_in(key, 11), NF, 1.0)).astype(jnp.bfloat16)


def draw_coarse_diag(key, part):
    return build_blocks(jax.random.fold_in(key, 23), NC, 4.0).astype(jnp.bfloat16)


def draw_coarse_smoother(key, part):
    return jnp.linalg.inv(build_blocks(jax.random.fold_in(key, 23), NC, 4.0)).astype(jnp.bfloat16)


def draw_fine_cols(key, part):
    return neighbour_columns(jax.random.fold_in(key, 37), NF, R_DEV // 2, R_DEV)


def draw_coarse_cols(key, part):
    return neighbour_columns(jax.random.fold_in(key, 41), NC, C_DEV // 2, C_DEV)


def draw_aggregate(key, part):
    row_ids = jnp.arange(NF, dtype=jnp.int32)
    owner_row = row_ids // R_DEV % N_ROWS
    local_slot = jax.random.randint(jax.random.fold_in(key, 53), (NF,), 0, C_DEV)
    local_slot = jnp.where(row_ids == 0, 0, jnp.where(row_ids == NF - 1, C_DEV - 1, local_slot))
    return (owner_row * C_DEV + local_slot).astype(jnp.int32)


def shard_levels(key, extent, cuts, smallest, largest):
    def one(axis_at, parts):
        draws = jax.random.uniform(jax.random.fold_in(jax.random.fold_in(key, 6), axis_at), (parts,), jnp.float32, smallest / len(cuts), largest / len(cuts))
        return jnp.repeat(jnp.exp(draws), extent[axis_at] // parts).reshape((-1,) + (1,) * (len(extent) - axis_at - 1))

    gain = one(*cuts[0])
    for cut in cuts[1:]:
        gain = gain * one(*cut)
    return gain


def centred(key, shape, width, most, cuts=(), kind=jnp.bfloat16):
    entries = jax.random.normal(key, shape, jnp.float32) * width
    if len(cuts) > 0:
        entries = shard_levels(key, shape, cuts, -0.22, 0.18) * entries
    return jnp.clip(entries, min=-most, max=most).astype(kind)


def setup_inputs(seed: int = 0) -> dict:
    seeds = jax.random.split(jax.random.key(seed), 11)
    rhs = centred(seeds[0], (NF, B, NRHS), 1.0, 6.0, ((0, 32),), jnp.float32)
    fine_diag = draw_fine_diag(jax.random.fold_in(seeds[10], 71), 0)
    fine_smoother = draw_fine_smoother(jax.random.fold_in(seeds[10], 71), 0)
    fine_blocks = centred(seeds[3], (NF, NEIGH, B, B), 0.03, 0.1796875, ((0, 32),))
    fine_cols = draw_fine_cols(jax.random.fold_in(seeds[10], 71), 0)
    aggregate = draw_aggregate(jax.random.fold_in(seeds[10], 71), 0)
    coarse_diag = draw_coarse_diag(jax.random.fold_in(seeds[10], 71), 0)
    coarse_smoother = draw_coarse_smoother(jax.random.fold_in(seeds[10], 71), 0)
    coarse_blocks = centred(seeds[8], (NC, NEIGH, B, B), 0.12, 0.71875, ((0, 8),))
    coarse_cols = draw_coarse_cols(jax.random.fold_in(seeds[10], 71), 0)
    return dict(rhs=rhs, fine_diag=fine_diag, fine_smoother=fine_smoother, fine_blocks=fine_blocks, fine_cols=fine_cols, aggregate=aggregate, coarse_diag=coarse_diag, coarse_smoother=coarse_smoother, coarse_blocks=coarse_blocks, coarse_cols=coarse_cols)


damping = 0.8

def rounded(values):
    return lax.optimization_barrier(values.astype(jnp.bfloat16)).astype(jnp.float32)

def block_product(blocks, vector):
    return jnp.einsum('nab,nbk->nak', blocks.astype(jnp.float32), rounded(vector), precision=lax.Precision.HIGHEST)

def apply_operator(diag_blocks, off_blocks, columns, vector, height):
    vector_low = rounded(vector)
    group_count = vector.shape[0] // height

    def one_group(group_index):
        first_row = group_index * height
        diag_part = lax.dynamic_slice_in_dim(diag_blocks, first_row, height, 0).astype(jnp.float32)
        off_part = lax.dynamic_slice_in_dim(off_blocks, first_row, height, 0).astype(jnp.float32)
        column_part = lax.dynamic_slice_in_dim(columns, first_row, height, 0)
        own_rows = lax.dynamic_slice_in_dim(vector_low, first_row, height, 0)
        nearby = jnp.take(vector_low, column_part, axis=0)
        own_term = jnp.einsum('nab,nbk->nak', diag_part, own_rows, precision=lax.Precision.HIGHEST)
        off_term = jnp.einsum('njab,njbk->nak', off_part, nearby, precision=lax.Precision.HIGHEST)
        return own_term + off_term
    result = lax.map(one_group, jnp.arange(group_count, dtype=jnp.int32))
    return result.reshape(vector.shape)

def reference(rhs, fine_diag, fine_smoother, fine_blocks, fine_cols, aggregate, coarse_diag, coarse_smoother, coarse_blocks, coarse_cols):
    first_iterate = damping * block_product(fine_smoother, rhs)
    first_residual = rhs - apply_operator(fine_diag, fine_blocks, fine_cols, first_iterate, R_DEV)
    second_iterate = first_iterate + damping * block_product(fine_smoother, first_residual)
    second_residual = rhs - apply_operator(fine_diag, fine_blocks, fine_cols, second_iterate, R_DEV)
    coarse_rhs = jax.ops.segment_sum(second_residual, aggregate, num_segments=NC)
    coarse_first = damping * block_product(coarse_smoother, coarse_rhs)
    coarse_image = apply_operator(coarse_diag, coarse_blocks, coarse_cols, coarse_first, C_DEV)
    coarse_second = coarse_first + damping * block_product(coarse_smoother, coarse_rhs - coarse_image)
    return second_iterate + jnp.take(coarse_second, aggregate, axis=0)
```

```python
import functools

import jax
import jax.numpy as jnp
from jax import lax
from jax.experimental import pallas as pl
from jax.experimental.pallas import tpu as pltpu
from jax.sharding import PartitionSpec as P

MESH = pl.DeviceIdType.MESH
damping = 0.8
low = jnp.bfloat16
f32 = jnp.float32


def dot(a, b):
    return jnp.dot(a, b, preferred_element_type=f32)


def row_product(i, columns, offs, diag, extended, own):
    count = offs.shape[1]
    vectors = [extended[columns[i, k]] for k in range(count)] + [extended[own]]
    blocks = [offs[i, k] for k in range(count)] + [diag[i]]
    total = None
    for at in range(0, count + 1, 4):
        term = dot(
            jnp.concatenate(blocks[at : at + 4], axis=1),
            jnp.concatenate(vectors[at : at + 4], axis=0),
        )
        total = term if total is None else total + term
    return total


def kernel(
    groups, ranks,
    fine_cols, coarse_cols, aggregate, chain,
    rhs_hbm, diag_hbm, smoother_hbm, blocks_hbm, cdiag_hbm, csmoother_hbm, cblocks_hbm,
    out_hbm,
    rhs, diag, smoother, blocks, cdiag, csmoother, cblocks,
    ext1, ext2, landing, iterate, sums, partial, from_partner, chip_send, chip_recv, crhs, cfirst, cext, correction,
    load_sem, out_sem, halo_send, halo_recv, rs_send, rs_recv, rc_send, rc_recv,
    piece_send, piece_recv, ag_send, ag_recv, fwd_send, fwd_recv,
):
    g = lax.axis_index("grp")
    r = lax.axis_index("rows")
    height = rhs.shape[0]
    margin = height // 2
    cheight = partial.shape[0]
    piece = cheight // groups
    chips = groups // 2
    reach = groups // 2
    steps = 4
    chunk = margin // steps

    flat = g * ranks + r
    has_left = flat > 0
    has_right = flat < groups * ranks - 1
    left = ((flat - 1) // ranks, (flat + ranks - 1) % ranks)
    right = ((flat + 1) // ranks, (flat + 1) % ranks)
    core = g % 2
    chip = g // 2
    partner = (chip * 2 + 1 - core, r)

    def piece_of(group, rank):
        odd = rank % 2
        return odd * (groups - 1 - group) + (1 - odd) * group

    q = piece_of(g, r)
    linear = r * groups + q

    def holder(index):
        rank = index // groups
        return (piece_of(index % groups, rank), rank)

    def chip_peer(o):
        return (((chip + o) % chips) * 2 + core, r)

    shifts = [d for s in range(1, reach + 1) for d in (s, -s)]

    def exists(index):
        return jnp.logical_and(index >= 0, index < groups * ranks)

    def load(src, dst, at):
        return pltpu.make_async_copy(src, dst, load_sem.at[at])

    mine = pl.ds(q * piece, piece)
    first_loads = [load(rhs_hbm, rhs, 0), load(smoother_hbm, smoother, 1)]
    later_loads = [
        load(blocks_hbm, blocks, 2),
        load(diag_hbm, diag, 3),
        load(csmoother_hbm.at[mine], csmoother, 4),
        load(cdiag_hbm.at[mine], cdiag, 5),
        load(cblocks_hbm.at[mine], cblocks, 6),
    ]
    for c in first_loads:
        c.start()

    barrier = pltpu.get_barrier_semaphore()

    def greet(device):
        pl.semaphore_signal(barrier, inc=1, device_id=device, device_id_type=MESH)

    pl.when(has_left)(lambda: greet(left))
    pl.when(has_right)(lambda: greet(right))
    greet(partner)
    for o in range(1, chips):
        greet(chip_peer(o))
    met = 1 + chips - 1 + has_left.astype(jnp.int32) + has_right.astype(jnp.int32)
    for d in shifts:
        there = exists(linear + d)
        pl.when(there)(functools.partial(lambda d: greet(holder(linear + d)), d))
        met = met + there.astype(jnp.int32)
    pl.semaphore_wait(barrier, met)

    def remote(src, dst, send, recv, device):
        return pltpu.make_async_remote_copy(
            src_ref=src, dst_ref=dst, send_sem=send, recv_sem=recv, device_id=device, device_id_type=MESH
        )

    def to_right(ext, phase, j):
        src = ext.at[pl.ds(margin + height - (j + 1) * chunk, chunk)]
        at = pl.ds(margin - (j + 1) * chunk, chunk)
        dst = landing.at[0, at] if phase == 0 else ext.at[at]
        return remote(src, dst, halo_send.at[phase, 0, j], halo_recv.at[phase, 0, j], right)

    def to_left(ext, phase, j):
        src = ext.at[pl.ds(margin + j * chunk, chunk)]
        at = pl.ds(j * chunk, chunk)
        dst = landing.at[1, at] if phase == 0 else ext.at[pl.ds(margin + height + j * chunk, chunk)]
        return remote(src, dst, halo_send.at[phase, 1, j], halo_recv.at[phase, 1, j], left)

    def send_halo(ext, phase, j):
        pl.when(has_right)(lambda: to_right(ext, phase, j).start())
        pl.when(has_left)(lambda: to_left(ext, phase, j).start())

    def wait_halo(ext, phase, j):
        pl.when(has_left)(lambda: to_right(ext, phase, j).wait_recv())
        pl.when(has_right)(lambda: to_left(ext, phase, j).wait_recv())

    def wait_sent(ext, phase, j):
        pl.when(has_right)(lambda: to_right(ext, phase, j).wait_send())
        pl.when(has_left)(lambda: to_left(ext, phase, j).wait_send())

    def rows(start, count, body, unroll):
        def step(n, carry):
            body(start + n)
            return carry

        lax.fori_loop(0, count, step, 0, unroll=unroll)

    for c in first_loads:
        c.wait()

    def first(i):
        value = damping * dot(smoother[i], rhs[i].astype(low))
        iterate[i] = value
        ext1[margin + i] = value.astype(low)

    for j in range(steps):
        rows(height - (j + 1) * chunk, chunk, first, 4)
        rows(j * chunk, chunk, first, 4)
        send_halo(ext1, 0, j)
    for c in later_loads:
        c.start()
    later_loads[0].wait()
    later_loads[1].wait()

    def second(i):
        residual = rhs[i] - row_product(i, fine_cols, blocks, diag, ext1, margin + i)
        value = iterate[i] + damping * dot(smoother[i], residual.astype(low))
        iterate[i] = value
        ext2[margin + i] = value.astype(low)

    def place_low(i):
        ext1[i] = landing[0, i]

    def place_high(i):
        ext1[margin + height + i] = landing[1, i]

    for j in range(steps):
        wait_halo(ext1, 0, j)
        pl.when(has_left)(lambda: rows(margin - (j + 1) * chunk, chunk, place_low, 4))
        pl.when(has_right)(lambda: rows(j * chunk, chunk, place_high, 4))
        rows(margin - (j + 1) * chunk, chunk, second, 2)
        rows(margin + j * chunk, chunk, second, 2)
        send_halo(ext2, 1, steps - 1 - j)

    for j in reversed(range(steps)):
        wait_halo(ext2, 1, j)
    sums[height] = jnp.zeros(sums.shape[1:], f32)

    def third(n):
        i = height - 1 - n
        residual = rhs[i] - row_product(i, fine_cols, blocks, diag, ext2, margin + i)
        sums[i] = residual + sums[chain[i]]

    rows(0, height, third, 2)

    def gather(c):
        partial[c] = sums[chain[height + c]]

    rows(0, cheight, gather, 4)

    def slice_of(group):
        return pl.ds(piece_of(group, r) * piece, piece)

    def to_partner(o):
        src = partial.at[slice_of(((chip + o) % chips) * 2 + 1 - core)]
        return remote(src, from_partner.at[o], rs_send.at[o], rs_recv.at[o], partner)

    order = [*range(1, chips), 0]
    for o in order:
        to_partner(o).start()

    def across(o):
        return remote(chip_send.at[o], chip_recv.at[o], rc_send.at[o], rc_recv.at[o], chip_peer(o))

    for o in order:
        to_partner(o).wait_recv()
        start = piece_of(((chip + o) % chips) * 2 + core, r) * piece
        if o:
            def pack(n):
                chip_send[o, n] = (partial[start + n] + from_partner[o, n]).astype(low)

            rows(0, piece, pack, 2)
            across(o).start()
        else:
            def keep(n):
                crhs[n] = partial[start + n] + from_partner[o, n]

            rows(0, piece, keep, 2)
    for c in later_loads[2:]:
        c.wait()
    for o in range(1, chips):
        across(o).wait_recv()

    def coarse_first(n):
        total = crhs[n]
        for o in range(1, chips):
            total = total + chip_recv[o, n].astype(f32)
        crhs[n] = total
        value = damping * dot(csmoother[n], total.astype(low))
        cfirst[n] = value
        cext[reach * piece + n] = value.astype(low)

    rows(0, piece, coarse_first, 2)

    def to_shift(d):
        at = shifts.index(d)
        return remote(
            cext.at[pl.ds(reach * piece, piece)], cext.at[pl.ds((reach - d) * piece, piece)],
            piece_send.at[at], piece_recv.at[at], holder(linear + d),
        )

    for d in reversed(shifts):
        pl.when(exists(linear + d))(functools.partial(lambda d: to_shift(d).start(), d))
    for d in reversed(shifts):
        pl.when(exists(linear - d))(functools.partial(lambda d: to_shift(d).wait_recv(), d))

    def coarse_second(n):
        image = row_product(q * piece + n, coarse_cols, cblocks_view, cdiag_view, cext, reach * piece + n)
        value = cfirst[n] + damping * dot(csmoother[n], (crhs[n] - image).astype(low))
        correction[q * piece + n] = value.astype(low)

    class Shifted:
        def __init__(self, ref):
            self.ref, self.shape = ref, ref.shape

        def __getitem__(self, at):
            if isinstance(at, tuple):
                return self.ref[(at[0] - q * piece, *at[1:])]
            return self.ref[at - q * piece]

    cblocks_view, cdiag_view = Shifted(cblocks), Shifted(cdiag)
    rows(0, piece, coarse_second, 2)

    def piece_to(o):
        return remote(correction.at[mine], correction.at[mine], ag_send.at[o], ag_recv.at[o], chip_peer(o))

    def forward(o):
        at = slice_of(((chip + o) % chips) * 2 + core)
        return remote(correction.at[at], correction.at[at], fwd_send.at[o], fwd_recv.at[o], partner)

    for o in range(1, chips):
        piece_to(o).start()
    forward(0).start()
    for o in range(1, chips):
        piece_to(o).wait_recv()
        forward((chips - o) % chips).start()
    for o in range(chips):
        forward(o).wait_recv()

    part = height // 4

    def final(i):
        iterate[i] = iterate[i] + correction[aggregate[i]].astype(f32)

    def put(j):
        at = pl.ds(j * part, part)
        return pltpu.make_async_copy(iterate.at[at], out_hbm.at[at], out_sem.at[j])

    for j in range(4):
        rows(j * part, part, final, 4)
        put(j).start()

    for j in range(steps):
        wait_sent(ext1, 0, j)
        wait_sent(ext2, 1, j)
    for o in range(chips):
        to_partner(o).wait_send()
        forward(o).wait_send()
    for o in range(1, chips):
        across(o).wait_send()
        piece_to(o).wait_send()
    for d in shifts:
        pl.when(exists(linear + d))(functools.partial(lambda d: to_shift(d).wait_send(), d))
    for j in range(4):
        put(j).wait()


def chain_table(local_index, coarse_height):
    height = local_index.shape[0]
    row = jnp.arange(height, dtype=jnp.int32)
    wanted = jnp.concatenate([local_index, jnp.arange(coarse_height, dtype=jnp.int32)])
    after = jnp.concatenate([row, jnp.full((coarse_height,), -1, jnp.int32)])
    hit = (wanted[:, None] == local_index[None, :]) & (row[None, :] > after[:, None])
    return jnp.min(jnp.where(hit, row[None, :], height), axis=1)


def on_device(
    groups, ranks,
    rhs, fine_diag, fine_smoother, fine_blocks, fine_cols, aggregate,
    coarse_diag, coarse_smoother, coarse_blocks, coarse_cols,
):
    height, b, n = rhs.shape
    cheight = coarse_diag.shape[0]
    neighbours = fine_blocks.shape[1]
    piece = cheight // groups
    chips = groups // 2
    reach = groups // 2
    g, r = lax.axis_index("grp"), lax.axis_index("rows")
    odd = r % 2
    q = odd * (groups - 1 - g) + (1 - odd) * g
    fine_cols = fine_cols - ((g * ranks + r) * height - height // 2)
    coarse_cols = coarse_cols - (r * groups + q - reach) * piece
    aggregate = aggregate - r * cheight
    table = chain_table(aggregate, cheight)
    vmem = pltpu.VMEM
    dma = pltpu.SemaphoreType.DMA
    smem = pl.BlockSpec(memory_space=pltpu.SMEM)
    hbm = pl.BlockSpec(memory_space=pl.ANY)
    return pl.pallas_call(
        functools.partial(kernel, groups, ranks),
        out_shape=jax.ShapeDtypeStruct(rhs.shape, f32),
        in_specs=[smem] * 4 + [hbm] * 7,
        out_specs=hbm,
        scratch_shapes=[
            vmem((height, b, n), f32),
            vmem((height, b, b), low),
            vmem((height, b, b), low),
            vmem((height, neighbours, b, b), low),
            vmem((piece, b, b), low),
            vmem((piece, b, b), low),
            vmem((piece, neighbours, b, b), low),
            vmem((2 * height, b, n), low),
            vmem((2 * height, b, n), low),
            vmem((2, height // 2, b, n), low),
            vmem((height, b, n), f32),
            vmem((height + 1, b, n), f32),
            vmem((cheight, b, n), f32),
            vmem((chips, piece, b, n), f32),
            vmem((chips, piece, b, n), low),
            vmem((chips, piece, b, n), low),
            vmem((piece, b, n), f32),
            vmem((piece, b, n), f32),
            vmem(((2 * reach + 1) * piece, b, n), low),
            vmem((cheight, b, n), low),
            dma((7,)),
            dma((4,)),
            dma((2, 2, 4)),
            dma((2, 2, 4)),
            dma((chips,)),
            dma((chips,)),
            dma((chips,)),
            dma((chips,)),
            dma((2 * reach,)),
            dma((2 * reach,)),
            dma((chips,)),
            dma((chips,)),
            dma((chips,)),
            dma((chips,)),
        ],
        compiler_params=pltpu.CompilerParams(
            collective_id=0, has_side_effects=True, vmem_limit_bytes=60 * 1024 * 1024
        ),
        name="cycle",
    )(
        fine_cols, coarse_cols, aggregate, table,
        rhs, fine_diag, fine_smoother, fine_blocks, coarse_diag, coarse_smoother, coarse_blocks,
    )


def solution(mesh):
    fine = P(("grp", "rows"))
    return jax.shard_map(
        functools.partial(on_device, mesh.shape["grp"], mesh.shape["rows"]),
        mesh=mesh,
        in_specs=(fine,) * 6 + (P("rows"),) * 4,
        out_specs=fine,
        check_vma=False,
    )
```

```python
import functools

import jax
import jax.numpy as jnp
import numpy as np
from jax import lax
from jax.experimental import pallas as pl
from jax.experimental.pallas import tpu as pltpu
from jax.sharding import PartitionSpec as P

MESH = pl.DeviceIdType.MESH
damping = 0.8
steps = 8
early = 1
parts = 4
low = jnp.bfloat16
f32 = jnp.float32


def dot(a, b):
    return jnp.dot(a, b, preferred_element_type=f32)


def row_product(i, columns, at, base, offs, diag, extended, own):
    count = offs.shape[1]
    last = extended.shape[0] - 1
    vectors = [extended[jnp.clip(columns[k, at] - base, 0, last)] for k in range(count)] + [extended[own]]
    blocks = [offs[i, k] for k in range(count)] + [diag[i]]
    total = None
    for p in range(0, count + 1, 4):
        term = dot(
            jnp.concatenate(blocks[p : p + 4], axis=1),
            jnp.concatenate(vectors[p : p + 4], axis=0),
        )
        total = term if total is None else total + term
    return total


def kernel(
    groups, ranks,
    fine_cols, coarse_cols, chain,
    rhs_hbm, diag_hbm, smoother_hbm, blocks_hbm, cdiag_hbm, csmoother_hbm, cblocks_hbm,
    iterate_hbm, correction_hbm,
    rhs, diag, smoother, blocks, cdiag, csmoother, cblocks,
    ext1, ext2, landing1, landing2, iterate, sums, partial, from_partner, chip_send, chip_recv, crhs, cfirst, cext, correction,
    load_sem, out_sem, halo_send, halo_recv, rs_send, rs_recv, rc_send, rc_recv,
    piece_send, piece_recv, ag_send, ag_recv, fwd_send, fwd_recv,
):
    g = lax.axis_index("grp")
    r = lax.axis_index("rows")
    height = rhs.shape[0]
    margin = height // 2
    cheight = partial.shape[0]
    piece = cheight // groups
    chips = groups // 2
    reach = groups // 2
    chunk = margin // steps
    share = piece // parts

    flat = g * ranks + r
    has_left = flat > 0
    has_right = flat < groups * ranks - 1
    left = ((flat - 1) // ranks, (flat + ranks - 1) % ranks)
    right = ((flat + 1) // ranks, (flat + 1) % ranks)
    core = g % 2
    chip = g // 2
    partner = (chip * 2 + 1 - core, r)

    def piece_of(group, rank):
        odd = rank % 2
        return odd * (groups - 1 - group) + (1 - odd) * group

    q = piece_of(g, r)
    linear = r * groups + q

    def holder(index):
        rank = index // groups
        return (piece_of(index % groups, rank), rank)

    def chip_peer(o):
        return (((chip + o) % chips) * 2 + core, r)

    shifts = [d for s in range(1, reach + 1) for d in (s, -s)]

    def exists(index):
        return jnp.logical_and(index >= 0, index < groups * ranks)

    def load(src, dst, at):
        return pltpu.make_async_copy(src, dst, load_sem.at[at])

    mine = pl.ds(q * piece, piece)
    first_loads = [load(rhs_hbm, rhs, 0), load(smoother_hbm, smoother, 1)]
    later_loads = [
        load(blocks_hbm, blocks, 2),
        load(diag_hbm, diag, 3),
        load(csmoother_hbm.at[mine], csmoother, 4),
        load(cdiag_hbm.at[mine], cdiag, 5),
        load(cblocks_hbm.at[mine], cblocks, 6),
    ]
    for c in first_loads:
        c.start()

    barrier = pltpu.get_barrier_semaphore()

    def greet(device):
        pl.semaphore_signal(barrier, inc=1, device_id=device, device_id_type=MESH)

    pl.when(has_left)(lambda: greet(left))
    pl.when(has_right)(lambda: greet(right))
    greet(partner)
    for o in range(1, chips):
        greet(chip_peer(o))
    met = 1 + chips - 1 + has_left.astype(jnp.int32) + has_right.astype(jnp.int32)
    for d in shifts:
        there = exists(linear + d)
        pl.when(there)(functools.partial(lambda d: greet(holder(linear + d)), d))
        met = met + there.astype(jnp.int32)
    pl.semaphore_wait(barrier, met)

    def remote(src, dst, send, recv, device):
        return pltpu.make_async_remote_copy(
            src_ref=src, dst_ref=dst, send_sem=send, recv_sem=recv, device_id=device, device_id_type=MESH
        )

    def to_right(ext, phase, j):
        src = ext.at[pl.ds(margin + height - (j + 1) * chunk, chunk)]
        at = pl.ds(margin - (j + 1) * chunk, chunk)
        dst = (landing1, landing2)[phase].at[0, at]
        return remote(src, dst, halo_send.at[phase, 0, j], halo_recv.at[phase, 0, j], right)

    def to_left(ext, phase, j):
        src = ext.at[pl.ds(margin + j * chunk, chunk)]
        at = pl.ds(j * chunk, chunk)
        dst = (landing1, landing2)[phase].at[1, at]
        return remote(src, dst, halo_send.at[phase, 1, j], halo_recv.at[phase, 1, j], left)

    def send_halo(ext, phase, j):
        pl.when(has_right)(lambda: to_right(ext, phase, j).start())
        pl.when(has_left)(lambda: to_left(ext, phase, j).start())

    def wait_halo(ext, phase, j):
        pl.when(has_left)(lambda: to_right(ext, phase, j).wait_recv())
        pl.when(has_right)(lambda: to_left(ext, phase, j).wait_recv())

    def wait_sent(ext, phase, j):
        pl.when(has_right)(lambda: to_right(ext, phase, j).wait_send())
        pl.when(has_left)(lambda: to_left(ext, phase, j).wait_send())

    def rows(start, count, body, unroll):
        def step(n, carry):
            body(start + n)
            return carry

        lax.fori_loop(0, count, step, 0, unroll=unroll)

    for c in first_loads:
        c.wait()

    def first(i):
        value = damping * dot(smoother[i], rhs[i].astype(low))
        iterate[i] = value
        ext1[margin + i] = value.astype(low)

    for j in range(steps):
        rows(height - (j + 1) * chunk, chunk, first, 4)
        rows(j * chunk, chunk, first, 4)
        send_halo(ext1, 0, j)
    for c in later_loads:
        c.start()
    later_loads[0].wait()
    later_loads[1].wait()

    def place(ext, landing, j):
        def place_low(i):
            ext[i] = landing[0, i]

        def place_high(i):
            ext[margin + height + i] = landing[1, i]

        pl.when(has_left)(lambda: rows(margin - (j + 1) * chunk, chunk, place_low, 4))
        pl.when(has_right)(lambda: rows(j * chunk, chunk, place_high, 4))

    base = flat * height - margin

    def second(i):
        residual = rhs[i] - row_product(i, fine_cols, i, base, blocks, diag, ext1, margin + i)
        value = iterate[i] + damping * dot(smoother[i], residual.astype(low))
        iterate[i] = value
        ext2[margin + i] = value.astype(low)

    for j in range(steps):
        wait_halo(ext1, 0, j)
        place(ext1, landing1, j)
        rows(margin - (j + 1) * chunk, chunk, second, 2)
        rows(margin + j * chunk, chunk, second, 2)
        if j < early:
            send_halo(ext2, 1, steps - 1 - j)
    for j in range(steps - early):
        send_halo(ext2, 1, j)
    keep_iterate = pltpu.make_async_copy(iterate, iterate_hbm, load_sem.at[7])
    keep_iterate.start()

    sums[0] = jnp.zeros(sums.shape[1:], f32)

    def third(shift):
        def body(i):
            residual = rhs[i] - row_product(i, fine_cols, i, base, blocks, diag, ext2, margin + i)
            sums[i + shift] = residual + sums[chain[i]]

        return body

    for j in reversed(range(steps - early, steps)):
        wait_halo(ext2, 1, j)
        place(ext2, landing2, j)
    for j in range(steps):
        if j < steps - early:
            wait_halo(ext2, 1, j)
            place(ext2, landing2, j)
        for n, start in enumerate((margin - (j + 1) * chunk, margin + j * chunk)):
            rows(start, chunk, third(1 + (2 * j + n) * chunk - start), 2)

    def gather(c):
        partial[c] = sums[chain[height + c]]

    rows(0, cheight, gather, 4)

    def slice_of(group, p):
        return pl.ds(piece_of(group, r) * piece + p * share, share)

    def to_partner(o, p):
        src = partial.at[slice_of(((chip + o) % chips) * 2 + 1 - core, p)]
        dst = from_partner.at[o, pl.ds(p * share, share)]
        return remote(src, dst, rs_send.at[o, p], rs_recv.at[o, p], partner)

    order = [*range(1, chips), 0]
    for o in order:
        for p in range(parts):
            to_partner(o, p).start()

    def across(o, p):
        at = pl.ds(p * share, share)
        return remote(chip_send.at[o, at], chip_recv.at[o, at], rc_send.at[o, p], rc_recv.at[o, p], chip_peer(o))

    for o in order:
        start = piece_of(((chip + o) % chips) * 2 + core, r) * piece

        def pack(n):
            chip_send[o, n] = (partial[start + n] + from_partner[o, n]).astype(low)

        def keep(n):
            crhs[n] = partial[start + n] + from_partner[o, n]

        for p in range(parts):
            to_partner(o, p).wait_recv()
            rows(p * share, share, pack if o else keep, 2)
            if o:
                across(o, p).start()
    for c in later_loads[2:]:
        c.wait()

    def coarse_first(n):
        total = crhs[n]
        for o in range(1, chips):
            total = total + chip_recv[o, n].astype(f32)
        crhs[n] = total
        value = damping * dot(csmoother[n], total.astype(low))
        cfirst[n] = value
        cext[reach * piece + n] = value.astype(low)

    def to_shift(d, p):
        at = shifts.index(d)
        return remote(
            cext.at[pl.ds(reach * piece + p * share, share)], cext.at[pl.ds((reach - d) * piece + p * share, share)],
            piece_send.at[at, p], piece_recv.at[at, p], holder(linear + d),
        )

    def each_part(method, d):
        for p in range(parts):
            getattr(to_shift(d, p), method)()

    for p in range(parts):
        for o in range(1, chips):
            across(o, p).wait_recv()
        rows(p * share, share, coarse_first, 2)
        for d in reversed(shifts):
            pl.when(exists(linear + d))(functools.partial(lambda d: to_shift(d, p).start(), d))
    for d in reversed(shifts):
        pl.when(exists(linear - d))(functools.partial(each_part, "wait_recv", d))

    cbase = (linear - reach) * piece

    def coarse_second(n):
        image = row_product(n, coarse_cols, q * piece + n, cbase, cblocks, cdiag, cext, reach * piece + n)
        value = cfirst[n] + damping * dot(csmoother[n], (crhs[n] - image).astype(low))
        correction[q * piece + n] = value.astype(low)

    def piece_to(o, p):
        at = slice_of(g, p)
        return remote(correction.at[at], correction.at[at], ag_send.at[o, p], ag_recv.at[o, p], chip_peer(o))

    def forward(o, p):
        at = slice_of(((chip + o) % chips) * 2 + core, p)
        return remote(correction.at[at], correction.at[at], fwd_send.at[o, p], fwd_recv.at[o, p], partner)

    def put(o, own, p):
        at = slice_of(((chip + o) % chips) * 2 + (core if own else 1 - core), p)
        return pltpu.make_async_copy(correction.at[at], correction_hbm.at[at], out_sem.at[o, own, p])

    for p in range(parts):
        rows(p * share, share, coarse_second, 2)
        for o in range(1, chips):
            piece_to(o, p).start()
        forward(0, p).start()
        put(0, 1, p).start()
    for o in range(1, chips):
        for p in range(parts):
            piece_to(o, p).wait_recv()
            forward(chips - o, p).start()
            put(chips - o, 1, p).start()
    for o in [0, *reversed(range(1, chips))]:
        for p in range(parts):
            forward(o, p).wait_recv()
            put(o, 0, p).start()

    for j in range(steps):
        wait_sent(ext1, 0, j)
        wait_sent(ext2, 1, j)
    for p in range(parts):
        for o in range(chips):
            to_partner(o, p).wait_send()
            forward(o, p).wait_send()
            put(o, 0, p).wait()
            put(o, 1, p).wait()
        for o in range(1, chips):
            across(o, p).wait_send()
            piece_to(o, p).wait_send()
    for d in shifts:
        pl.when(exists(linear + d))(functools.partial(each_part, "wait_send", d))
    keep_iterate.wait()


def add_kernel(cheight, aggregate, iterate, correction, out):
    count = out.shape[0]
    first = pl.program_id(0) * count
    start = lax.axis_index("rows") * cheight

    def step(n, carry):
        out[n] = iterate[n] + correction[aggregate[first + n] - start].astype(f32)
        return carry

    lax.fori_loop(0, count, step, 0, unroll=4)


def chain_table(aggregate, first_coarse, coarse_height, chunk):
    height = aggregate.shape[0]
    margin = height // 2
    row = np.arange(height)
    j = np.where(row < margin, margin - 1 - row, row - margin) // chunk
    start = np.where(row < margin, margin - (j + 1) * chunk, margin + j * chunk)
    slot = (1 + 2 * j * chunk + np.where(row < margin, 0, chunk) + row - start).astype(np.int32)
    limit = np.concatenate([slot, np.full(coarse_height, height + 1, np.int32)])
    wanted = jnp.concatenate([aggregate, first_coarse + jnp.arange(coarse_height, dtype=jnp.int32)])
    hit = (wanted[:, None] == aggregate[None, :]) & (slot[None, :] < limit[:, None])
    return jnp.max(jnp.where(hit, slot[None, :], 0), axis=1)


def on_device(
    groups, ranks,
    rhs, fine_diag, fine_smoother, fine_blocks, fine_cols, aggregate,
    coarse_diag, coarse_smoother, coarse_blocks, coarse_cols,
):
    height, b, n = rhs.shape
    cheight = coarse_diag.shape[0]
    neighbours = fine_blocks.shape[1]
    piece = cheight // groups
    chips = groups // 2
    reach = groups // 2
    chunk = height // 2 // steps
    table = chain_table(aggregate, lax.axis_index("rows") * cheight, cheight, chunk)
    vmem = pltpu.VMEM
    dma = pltpu.SemaphoreType.DMA
    smem = pl.BlockSpec(memory_space=pltpu.SMEM)
    hbm = pl.BlockSpec(memory_space=pl.ANY)
    iterate, correction = pl.pallas_call(
        functools.partial(kernel, groups, ranks),
        out_shape=(jax.ShapeDtypeStruct(rhs.shape, f32), jax.ShapeDtypeStruct((cheight, b, n), low)),
        in_specs=[smem] * 3 + [hbm] * 7,
        out_specs=(hbm, hbm),
        scratch_shapes=[
            vmem((height, b, n), f32),
            vmem((height, b, b), low),
            vmem((height, b, b), low),
            vmem((height, neighbours, b, b), low),
            vmem((piece, b, b), low),
            vmem((piece, b, b), low),
            vmem((piece, neighbours, b, b), low),
            vmem((2 * height, b, n), low),
            vmem((2 * height, b, n), low),
            vmem((2, height // 2, b, n), low),
            vmem((2, height // 2, b, n), low),
            vmem((height, b, n), f32),
            vmem((height + 1, b, n), f32),
            vmem((cheight, b, n), f32),
            vmem((chips, piece, b, n), f32),
            vmem((chips, piece, b, n), low),
            vmem((chips, piece, b, n), low),
            vmem((piece, b, n), f32),
            vmem((piece, b, n), f32),
            vmem(((2 * reach + 1) * piece, b, n), low),
            vmem((cheight, b, n), low),
            dma((8,)),
            dma((chips, 2, parts)),
            dma((2, 2, steps)),
            dma((2, 2, steps)),
            dma((chips, parts)),
            dma((chips, parts)),
            dma((chips, parts)),
            dma((chips, parts)),
            dma((2 * reach, parts)),
            dma((2 * reach, parts)),
            dma((chips, parts)),
            dma((chips, parts)),
            dma((chips, parts)),
            dma((chips, parts)),
        ],
        compiler_params=pltpu.CompilerParams(
            collective_id=0, has_side_effects=True, vmem_limit_bytes=60 * 1024 * 1024
        ),
        name="cycle",
    )(
        fine_cols.T, coarse_cols.T, table,
        rhs, fine_diag, fine_smoother, fine_blocks, coarse_diag, coarse_smoother, coarse_blocks,
    )
    share = height // 8
    return pl.pallas_call(
        functools.partial(add_kernel, cheight),
        out_shape=jax.ShapeDtypeStruct(rhs.shape, f32),
        grid=(height // share,),
        in_specs=[
            smem,
            pl.BlockSpec((share, b, n), lambda i: (i, 0, 0)),
            pl.BlockSpec((cheight, b, n), lambda i: (0, 0, 0)),
        ],
        out_specs=pl.BlockSpec((share, b, n), lambda i: (i, 0, 0)),
        name="add",
    )(aggregate, iterate, correction)


def solution(mesh):
    fine = P(("grp", "rows"))
    return jax.shard_map(
        functools.partial(on_device, mesh.shape["grp"], mesh.shape["rows"]),
        mesh=mesh,
        in_specs=(fine,) * 6 + (P("rows"),) * 4,
        out_specs=fine,
        check_vma=False,
    )
```

```python
import functools

import jax
import jax.numpy as jnp
from jax import lax
from jax.experimental import pallas as pl
from jax.experimental.pallas import tpu as pltpu
from jax.sharding import PartitionSpec as P

MESH = pl.DeviceIdType.MESH
damping = 0.8
steps = 8
early = 1
parts = 4
low = jnp.bfloat16
f32 = jnp.float32


def dot(a, b):
    return jnp.dot(a, b, preferred_element_type=f32)


def row_product(i, columns, at, base, offs, diag, extended, own):
    count = offs.shape[1]
    last = extended.shape[0] - 1
    vectors = [extended[jnp.clip(columns[k, at] - base, 0, last)] for k in range(count)] + [extended[own]]
    blocks = [offs[i, k] for k in range(count)] + [diag[i]]
    total = None
    for p in range(0, count + 1, 4):
        term = dot(
            jnp.concatenate(blocks[p : p + 4], axis=1),
            jnp.concatenate(vectors[p : p + 4], axis=0),
        )
        total = term if total is None else total + term
    return total


def kernel(
    groups, ranks,
    fine_cols, coarse_cols, aggregate,
    rhs_hbm, diag_hbm, smoother_hbm, blocks_hbm, cdiag_hbm, csmoother_hbm, cblocks_hbm,
    iterate_hbm, correction_hbm,
    rhs, diag, smoother, blocks, cdiag, csmoother, cblocks,
    ext1, ext2, landing1, landing2, iterate, sums, partial, from_partner, chip_send, chip_recv, crhs, cfirst, cext, correction, chain,
    load_sem, out_sem, halo_send, halo_recv, rs_send, rs_recv, rc_send, rc_recv,
    piece_send, piece_recv, ag_send, ag_recv, fwd_send, fwd_recv,
):
    g = lax.axis_index("grp")
    r = lax.axis_index("rows")
    height = rhs.shape[0]
    margin = height // 2
    cheight = partial.shape[0]
    piece = cheight // groups
    chips = groups // 2
    reach = groups // 2
    chunk = margin // steps
    share = piece // parts

    flat = g * ranks + r
    has_left = flat > 0
    has_right = flat < groups * ranks - 1
    left = ((flat - 1) // ranks, (flat + ranks - 1) % ranks)
    right = ((flat + 1) // ranks, (flat + 1) % ranks)
    core = g % 2
    chip = g // 2
    partner = (chip * 2 + 1 - core, r)

    def piece_of(group, rank):
        odd = rank % 2
        return odd * (groups - 1 - group) + (1 - odd) * group

    q = piece_of(g, r)
    linear = r * groups + q

    def holder(index):
        rank = index // groups
        return (piece_of(index % groups, rank), rank)

    def chip_peer(o):
        return (((chip + o) % chips) * 2 + core, r)

    shifts = [d for s in range(1, reach + 1) for d in (s, -s)]

    def exists(index):
        return jnp.logical_and(index >= 0, index < groups * ranks)

    def load(src, dst, at):
        return pltpu.make_async_copy(src, dst, load_sem.at[at])

    mine = pl.ds(q * piece, piece)
    first_loads = [load(rhs_hbm, rhs, 0), load(smoother_hbm, smoother, 1)]
    later_loads = [
        load(blocks_hbm, blocks, 2),
        load(diag_hbm, diag, 3),
        load(csmoother_hbm.at[mine], csmoother, 4),
        load(cdiag_hbm.at[mine], cdiag, 5),
        load(cblocks_hbm.at[mine], cblocks, 6),
    ]
    for c in first_loads:
        c.start()

    barrier = pltpu.get_barrier_semaphore()

    def greet(device):
        pl.semaphore_signal(barrier, inc=1, device_id=device, device_id_type=MESH)

    pl.when(has_left)(lambda: greet(left))
    pl.when(has_right)(lambda: greet(right))
    greet(partner)
    for o in range(1, chips):
        greet(chip_peer(o))
    met = 1 + chips - 1 + has_left.astype(jnp.int32) + has_right.astype(jnp.int32)
    for d in shifts:
        there = exists(linear + d)
        pl.when(there)(functools.partial(lambda d: greet(holder(linear + d)), d))
        met = met + there.astype(jnp.int32)
    pl.semaphore_wait(barrier, met)

    def remote(src, dst, send, recv, device):
        return pltpu.make_async_remote_copy(
            src_ref=src, dst_ref=dst, send_sem=send, recv_sem=recv, device_id=device, device_id_type=MESH
        )

    def to_right(ext, phase, j):
        src = ext.at[pl.ds(margin + height - (j + 1) * chunk, chunk)]
        at = pl.ds(margin - (j + 1) * chunk, chunk)
        dst = (landing1, landing2)[phase].at[0, at]
        return remote(src, dst, halo_send.at[phase, 0, j], halo_recv.at[phase, 0, j], right)

    def to_left(ext, phase, j):
        src = ext.at[pl.ds(margin + j * chunk, chunk)]
        at = pl.ds(j * chunk, chunk)
        dst = (landing1, landing2)[phase].at[1, at]
        return remote(src, dst, halo_send.at[phase, 1, j], halo_recv.at[phase, 1, j], left)

    def send_halo(ext, phase, j):
        pl.when(has_right)(lambda: to_right(ext, phase, j).start())
        pl.when(has_left)(lambda: to_left(ext, phase, j).start())

    def wait_halo(ext, phase, j):
        pl.when(has_left)(lambda: to_right(ext, phase, j).wait_recv())
        pl.when(has_right)(lambda: to_left(ext, phase, j).wait_recv())

    def wait_sent(ext, phase, j):
        pl.when(has_right)(lambda: to_right(ext, phase, j).wait_send())
        pl.when(has_left)(lambda: to_left(ext, phase, j).wait_send())

    def rows(start, count, body, unroll):
        def step(n, carry):
            body(start + n)
            return carry

        lax.fori_loop(0, count, step, 0, unroll=unroll)

    for c in first_loads:
        c.wait()

    def first(i):
        value = damping * dot(smoother[i], rhs[i].astype(low))
        iterate[i] = value
        ext1[margin + i] = value.astype(low)

    for j in range(steps):
        rows(height - (j + 1) * chunk, chunk, first, 4)
        rows(j * chunk, chunk, first, 4)
        send_halo(ext1, 0, j)
    for c in later_loads:
        c.start()
    starts = [at for j in range(steps) for at in (margin - (j + 1) * chunk, margin + j * chunk)]

    def earlier(wanted, runs):
        found = jnp.int32(0)
        for n in range(runs):
            for m in range(chunk):
                found = jnp.where(aggregate[starts[n] + m] == wanted, 1 + n * chunk + m, found)
        return found

    def link_run(n):
        def link(m):
            wanted = aggregate[starts[n] + m]
            found = earlier(wanted, n)
            for k in range(chunk - 1):
                same = jnp.logical_and(aggregate[starts[n] + k] == wanted, k < m)
                found = jnp.where(same, 1 + n * chunk + k, found)
            chain[starts[n] + m] = found

        rows(0, chunk, link, 1)

    def link_coarse(c):
        chain[height + c] = earlier(r * cheight + c, len(starts))

    def place(ext, landing, j):
        def place_low(i):
            ext[i] = landing[0, i]

        def place_high(i):
            ext[margin + height + i] = landing[1, i]

        pl.when(has_left)(lambda: rows(margin - (j + 1) * chunk, chunk, place_low, 4))
        pl.when(has_right)(lambda: rows(j * chunk, chunk, place_high, 4))

    rows(0, cheight // 2, link_coarse, 1)
    later_loads[0].wait()
    later_loads[1].wait()

    base = flat * height - margin

    def second(i):
        residual = rhs[i] - row_product(i, fine_cols, i, base, blocks, diag, ext1, margin + i)
        value = iterate[i] + damping * dot(smoother[i], residual.astype(low))
        iterate[i] = value
        ext2[margin + i] = value.astype(low)

    for j in range(steps):
        wait_halo(ext1, 0, j)
        place(ext1, landing1, j)
        rows(margin - (j + 1) * chunk, chunk, second, 2)
        rows(margin + j * chunk, chunk, second, 2)
        if j < early:
            send_halo(ext2, 1, steps - 1 - j)
        if j < steps - 1:
            link_run(2 * j)
            link_run(2 * j + 1)
    for j in range(steps - early):
        send_halo(ext2, 1, j)
    keep_iterate = pltpu.make_async_copy(iterate, iterate_hbm, load_sem.at[7])
    keep_iterate.start()
    link_run(2 * steps - 2)
    link_run(2 * steps - 1)

    sums[0] = jnp.zeros(sums.shape[1:], f32)

    def third(shift):
        def body(i):
            residual = rhs[i] - row_product(i, fine_cols, i, base, blocks, diag, ext2, margin + i)
            sums[i + shift] = residual + sums[chain[i]]

        return body

    for j in reversed(range(steps - early, steps)):
        wait_halo(ext2, 1, j)
        place(ext2, landing2, j)
    for j in range(steps):
        if j < steps - early:
            wait_halo(ext2, 1, j)
            place(ext2, landing2, j)
        for n, start in enumerate((margin - (j + 1) * chunk, margin + j * chunk)):
            rows(start, chunk, third(1 + (2 * j + n) * chunk - start), 2)
        if j < 4:
            rows(cheight // 2 + j * (cheight // 8), cheight // 8, link_coarse, 1)

    def gather(c):
        partial[c] = sums[chain[height + c]]

    rows(0, cheight, gather, 4)

    def slice_of(group, p):
        return pl.ds(piece_of(group, r) * piece + p * share, share)

    def to_partner(o, p):
        src = partial.at[slice_of(((chip + o) % chips) * 2 + 1 - core, p)]
        dst = from_partner.at[o, pl.ds(p * share, share)]
        return remote(src, dst, rs_send.at[o, p], rs_recv.at[o, p], partner)

    order = [*range(1, chips), 0]
    for o in order:
        for p in range(parts):
            to_partner(o, p).start()

    def across(o, p):
        at = pl.ds(p * share, share)
        return remote(chip_send.at[o, at], chip_recv.at[o, at], rc_send.at[o, p], rc_recv.at[o, p], chip_peer(o))

    for o in order:
        start = piece_of(((chip + o) % chips) * 2 + core, r) * piece

        def pack(n):
            chip_send[o, n] = (partial[start + n] + from_partner[o, n]).astype(low)

        def keep(n):
            crhs[n] = partial[start + n] + from_partner[o, n]

        for p in range(parts):
            to_partner(o, p).wait_recv()
            rows(p * share, share, pack if o else keep, 2)
            if o:
                across(o, p).start()
    for c in later_loads[2:]:
        c.wait()

    def coarse_first(n):
        total = crhs[n]
        for o in range(1, chips):
            total = total + chip_recv[o, n].astype(f32)
        crhs[n] = total
        value = damping * dot(csmoother[n], total.astype(low))
        cfirst[n] = value
        cext[reach * piece + n] = value.astype(low)

    def to_shift(d, p):
        at = shifts.index(d)
        return remote(
            cext.at[pl.ds(reach * piece + p * share, share)], cext.at[pl.ds((reach - d) * piece + p * share, share)],
            piece_send.at[at, p], piece_recv.at[at, p], holder(linear + d),
        )

    def each_part(method, d):
        for p in range(parts):
            getattr(to_shift(d, p), method)()

    for p in range(parts):
        for o in range(1, chips):
            across(o, p).wait_recv()
        rows(p * share, share, coarse_first, 2)
        for d in reversed(shifts):
            pl.when(exists(linear + d))(functools.partial(lambda d: to_shift(d, p).start(), d))
    for d in reversed(shifts):
        pl.when(exists(linear - d))(functools.partial(each_part, "wait_recv", d))

    cbase = (linear - reach) * piece

    def coarse_second(n):
        image = row_product(n, coarse_cols, q * piece + n, cbase, cblocks, cdiag, cext, reach * piece + n)
        value = cfirst[n] + damping * dot(csmoother[n], (crhs[n] - image).astype(low))
        correction[q * piece + n] = value.astype(low)

    def piece_to(o, p):
        at = slice_of(g, p)
        return remote(correction.at[at], correction.at[at], ag_send.at[o, p], ag_recv.at[o, p], chip_peer(o))

    def forward(o, p):
        at = slice_of(((chip + o) % chips) * 2 + core, p)
        return remote(correction.at[at], correction.at[at], fwd_send.at[o, p], fwd_recv.at[o, p], partner)

    def put(o, own, p):
        at = slice_of(((chip + o) % chips) * 2 + (core if own else 1 - core), p)
        return pltpu.make_async_copy(correction.at[at], correction_hbm.at[at], out_sem.at[o, own, p])

    for p in range(parts):
        rows(p * share, share, coarse_second, 2)
        for o in range(1, chips):
            piece_to(o, p).start()
        forward(0, p).start()
        put(0, 1, p).start()
    for o in range(1, chips):
        for p in range(parts):
            piece_to(o, p).wait_recv()
            forward(chips - o, p).start()
            put(chips - o, 1, p).start()
    for o in [0, *reversed(range(1, chips))]:
        for p in range(parts):
            forward(o, p).wait_recv()
            put(o, 0, p).start()

    for j in range(steps):
        wait_sent(ext1, 0, j)
        wait_sent(ext2, 1, j)
    for p in range(parts):
        for o in range(chips):
            to_partner(o, p).wait_send()
            forward(o, p).wait_send()
            put(o, 0, p).wait()
            put(o, 1, p).wait()
        for o in range(1, chips):
            across(o, p).wait_send()
            piece_to(o, p).wait_send()
    for d in shifts:
        pl.when(exists(linear + d))(functools.partial(each_part, "wait_send", d))
    keep_iterate.wait()


def add_kernel(
    cheight, aggregate, iterate_hbm, correction_hbm, out_hbm, iterate, correction, in_sem, correction_sem, out_sem
):
    share = iterate.shape[0] // 4
    cshare = cheight // 4
    start = lax.axis_index("rows") * cheight

    def fetch(j):
        at = pl.ds(j * cshare, cshare)
        return pltpu.make_async_copy(correction_hbm.at[at], correction.at[at], correction_sem.at[j])

    def get(j):
        at = pl.ds(j * share, share)
        return pltpu.make_async_copy(iterate_hbm.at[at], iterate.at[at], in_sem.at[j])

    def put(j):
        at = pl.ds(j * share, share)
        return pltpu.make_async_copy(iterate.at[at], out_hbm.at[at], out_sem.at[j])

    for j in range(4):
        fetch(j).start()
    for j in range(4):
        get(j).start()
    for j in range(4):
        fetch(j).wait()
    for j in range(4):
        get(j).wait()

        def step(n, carry):
            i = j * share + n
            iterate[i] = iterate[i] + correction[aggregate[i] - start].astype(f32)
            return carry

        lax.fori_loop(0, share, step, 0, unroll=4)
        put(j).start()
    for j in range(4):
        put(j).wait()


def on_device(
    groups, ranks,
    rhs, fine_diag, fine_smoother, fine_blocks, fine_cols, aggregate,
    coarse_diag, coarse_smoother, coarse_blocks, coarse_cols,
):
    height, b, n = rhs.shape
    cheight = coarse_diag.shape[0]
    neighbours = fine_blocks.shape[1]
    piece = cheight // groups
    chips = groups // 2
    reach = groups // 2
    vmem = pltpu.VMEM
    dma = pltpu.SemaphoreType.DMA
    smem = pl.BlockSpec(memory_space=pltpu.SMEM)
    hbm = pl.BlockSpec(memory_space=pl.ANY)
    iterate, correction = pl.pallas_call(
        functools.partial(kernel, groups, ranks),
        out_shape=(jax.ShapeDtypeStruct(rhs.shape, f32), jax.ShapeDtypeStruct((cheight, b, n), low)),
        in_specs=[smem] * 3 + [hbm] * 7,
        out_specs=(hbm, hbm),
        scratch_shapes=[
            vmem((height, b, n), f32),
            vmem((height, b, b), low),
            vmem((height, b, b), low),
            vmem((height, neighbours, b, b), low),
            vmem((piece, b, b), low),
            vmem((piece, b, b), low),
            vmem((piece, neighbours, b, b), low),
            vmem((2 * height, b, n), low),
            vmem((2 * height, b, n), low),
            vmem((2, height // 2, b, n), low),
            vmem((2, height // 2, b, n), low),
            vmem((height, b, n), f32),
            vmem((height + 1, b, n), f32),
            vmem((cheight, b, n), f32),
            vmem((chips, piece, b, n), f32),
            vmem((chips, piece, b, n), low),
            vmem((chips, piece, b, n), low),
            vmem((piece, b, n), f32),
            vmem((piece, b, n), f32),
            vmem(((2 * reach + 1) * piece, b, n), low),
            vmem((cheight, b, n), low),
            pltpu.SMEM((height + cheight,), jnp.int32),
            dma((8,)),
            dma((chips, 2, parts)),
            dma((2, 2, steps)),
            dma((2, 2, steps)),
            dma((chips, parts)),
            dma((chips, parts)),
            dma((chips, parts)),
            dma((chips, parts)),
            dma((2 * reach, parts)),
            dma((2 * reach, parts)),
            dma((chips, parts)),
            dma((chips, parts)),
            dma((chips, parts)),
            dma((chips, parts)),
        ],
        compiler_params=pltpu.CompilerParams(
            collective_id=0, has_side_effects=True, vmem_limit_bytes=60 * 1024 * 1024
        ),
        name="cycle",
    )(
        fine_cols.T, coarse_cols.T, aggregate,
        rhs, fine_diag, fine_smoother, fine_blocks, coarse_diag, coarse_smoother, coarse_blocks,
    )
    return pl.pallas_call(
        functools.partial(add_kernel, cheight),
        out_shape=jax.ShapeDtypeStruct(rhs.shape, f32),
        in_specs=[smem, hbm, hbm],
        out_specs=hbm,
        scratch_shapes=[vmem((height, b, n), f32), vmem((cheight, b, n), low), dma((4,)), dma((4,)), dma((4,))],
        name="add",
    )(aggregate, iterate, correction)


def solution(mesh):
    fine = P(("grp", "rows"))
    return jax.shard_map(
        functools.partial(on_device, mesh.shape["grp"], mesh.shape["rows"]),
        mesh=mesh,
        in_specs=(fine,) * 6 + (P("rows"),) * 4,
        out_specs=fine,
        check_vma=False,
    )
```

```python
import functools

import jax
import jax.numpy as jnp
from jax import lax
from jax.experimental import pallas as pl
from jax.experimental.pallas import tpu as pltpu
from jax.sharding import PartitionSpec as P

MESH = pl.DeviceIdType.MESH
damping = 0.8
steps = 8
early = 1
parts = 4
low = jnp.bfloat16
f32 = jnp.float32


def dot(a, b):
    return jnp.dot(a, b, preferred_element_type=f32)


def row_product(i, columns, at, base, offs, diag, extended, own):
    count = offs.shape[1]
    last = extended.shape[0] - 1
    vectors = [extended[jnp.clip(columns[k, at] - base, 0, last)] for k in range(count)] + [extended[own]]
    blocks = [offs[i, k] for k in range(count)] + [diag[i]]
    total = None
    for p in range(0, count + 1, 4):
        term = dot(
            jnp.concatenate(blocks[p : p + 4], axis=1),
            jnp.concatenate(vectors[p : p + 4], axis=0),
        )
        total = term if total is None else total + term
    return total


def kernel(
    groups, ranks,
    fine_cols, coarse_cols, aggregate,
    rhs_hbm, diag_hbm, smoother_hbm, blocks_hbm, cdiag_hbm, csmoother_hbm, cblocks_hbm,
    iterate_hbm, correction_hbm,
    rhs, diag, smoother, blocks, cdiag, csmoother, cblocks,
    ext1, ext2, landing1, landing2, iterate, sums, partial, from_partner, chip_send, chip_recv, crhs, cfirst, cext, correction, chain,
    load_sem, out_sem, halo_send, halo_recv, rs_send, rs_recv, rc_send, rc_recv,
    piece_send, piece_recv, ag_send, ag_recv, fwd_send, fwd_recv,
):
    g = lax.axis_index("grp")
    r = lax.axis_index("rows")
    height = rhs.shape[0]
    margin = height // 2
    cheight = partial.shape[0]
    piece = cheight // groups
    chips = groups // 2
    reach = groups // 2
    chunk = margin // steps
    share = piece // parts

    flat = g * ranks + r
    has_left = flat > 0
    has_right = flat < groups * ranks - 1
    left = ((flat - 1) // ranks, (flat + ranks - 1) % ranks)
    right = ((flat + 1) // ranks, (flat + 1) % ranks)
    core = g % 2
    chip = g // 2
    partner = (chip * 2 + 1 - core, r)

    def piece_of(group, rank):
        odd = rank % 2
        return odd * (groups - 1 - group) + (1 - odd) * group

    q = piece_of(g, r)
    linear = r * groups + q

    def holder(index):
        rank = index // groups
        return (piece_of(index % groups, rank), rank)

    def chip_peer(o):
        return (((chip + o) % chips) * 2 + core, r)

    shifts = [d for s in range(1, reach + 1) for d in (s, -s)]

    def exists(index):
        return jnp.logical_and(index >= 0, index < groups * ranks)

    def load(src, dst, at):
        return pltpu.make_async_copy(src, dst, load_sem.at[at])

    mine = pl.ds(q * piece, piece)
    first_loads = [load(rhs_hbm, rhs, 0), load(smoother_hbm, smoother, 1)]
    later_loads = [
        load(blocks_hbm, blocks, 2),
        load(diag_hbm, diag, 3),
        load(csmoother_hbm.at[mine], csmoother, 4),
        load(cdiag_hbm.at[mine], cdiag, 5),
        load(cblocks_hbm.at[mine], cblocks, 6),
    ]
    for c in first_loads:
        c.start()

    barrier = pltpu.get_barrier_semaphore()

    def greet(device):
        pl.semaphore_signal(barrier, inc=1, device_id=device, device_id_type=MESH)

    pl.when(has_left)(lambda: greet(left))
    pl.when(has_right)(lambda: greet(right))
    greet(partner)
    for o in range(1, chips):
        greet(chip_peer(o))
    met = 1 + chips - 1 + has_left.astype(jnp.int32) + has_right.astype(jnp.int32)
    for d in shifts:
        there = exists(linear + d)
        pl.when(there)(functools.partial(lambda d: greet(holder(linear + d)), d))
        met = met + there.astype(jnp.int32)
    pl.semaphore_wait(barrier, met)

    def remote(src, dst, send, recv, device):
        return pltpu.make_async_remote_copy(
            src_ref=src, dst_ref=dst, send_sem=send, recv_sem=recv, device_id=device, device_id_type=MESH
        )

    def to_right(ext, phase, j):
        src = ext.at[pl.ds(margin + height - (j + 1) * chunk, chunk)]
        at = pl.ds(margin - (j + 1) * chunk, chunk)
        dst = (landing1, landing2)[phase].at[0, at]
        return remote(src, dst, halo_send.at[phase, 0, j], halo_recv.at[phase, 0, j], right)

    def to_left(ext, phase, j):
        src = ext.at[pl.ds(margin + j * chunk, chunk)]
        at = pl.ds(j * chunk, chunk)
        dst = (landing1, landing2)[phase].at[1, at]
        return remote(src, dst, halo_send.at[phase, 1, j], halo_recv.at[phase, 1, j], left)

    def send_halo(ext, phase, j):
        pl.when(has_right)(lambda: to_right(ext, phase, j).start())
        pl.when(has_left)(lambda: to_left(ext, phase, j).start())

    def wait_halo(ext, phase, j):
        pl.when(has_left)(lambda: to_right(ext, phase, j).wait_recv())
        pl.when(has_right)(lambda: to_left(ext, phase, j).wait_recv())

    def wait_sent(ext, phase, j):
        pl.when(has_right)(lambda: to_right(ext, phase, j).wait_send())
        pl.when(has_left)(lambda: to_left(ext, phase, j).wait_send())

    def rows(start, count, body, unroll):
        def step(n, carry):
            body(start + n)
            return carry

        lax.fori_loop(0, count, step, 0, unroll=unroll)

    for c in first_loads:
        c.wait()

    def first(i):
        value = damping * dot(smoother[i], rhs[i].astype(low))
        iterate[i] = value
        ext1[margin + i] = value.astype(low)

    for j in range(steps):
        rows(height - (j + 1) * chunk, chunk, first, 4)
        rows(j * chunk, chunk, first, 4)
        send_halo(ext1, 0, j)
    for c in later_loads:
        c.start()
    starts = [at for j in range(steps) for at in (margin - (j + 1) * chunk, margin + j * chunk)]

    def earlier(wanted, runs):
        found = jnp.int32(0)
        for n in range(runs):
            for m in range(chunk):
                found = jnp.where(aggregate[starts[n] + m] == wanted, 1 + n * chunk + m, found)
        return found

    def link_run(n):
        def link(m):
            wanted = aggregate[starts[n] + m]
            found = earlier(wanted, n)
            for k in range(chunk - 1):
                same = jnp.logical_and(aggregate[starts[n] + k] == wanted, k < m)
                found = jnp.where(same, 1 + n * chunk + k, found)
            chain[starts[n] + m] = found

        rows(0, chunk, link, 1)

    def link_coarse(c):
        chain[height + c] = earlier(r * cheight + c, len(starts))

    def place(ext, landing, j):
        def place_low(i):
            ext[i] = landing[0, i]

        def place_high(i):
            ext[margin + height + i] = landing[1, i]

        pl.when(has_left)(lambda: rows(margin - (j + 1) * chunk, chunk, place_low, 4))
        pl.when(has_right)(lambda: rows(j * chunk, chunk, place_high, 4))

    rows(0, cheight // 4, link_coarse, 1)
    later_loads[0].wait()
    later_loads[1].wait()

    base = flat * height - margin

    def second(i):
        residual = rhs[i] - row_product(i, fine_cols, i, base, blocks, diag, ext1, margin + i)
        value = iterate[i] + damping * dot(smoother[i], residual.astype(low))
        iterate[i] = value
        ext2[margin + i] = value.astype(low)

    for j in range(steps):
        wait_halo(ext1, 0, j)
        place(ext1, landing1, j)
        rows(margin - (j + 1) * chunk, chunk, second, 2)
        rows(margin + j * chunk, chunk, second, 2)
        if j < early:
            send_halo(ext2, 1, steps - 1 - j)
        if j < steps - 1:
            link_run(2 * j)
            link_run(2 * j + 1)
    for j in range(steps - early):
        send_halo(ext2, 1, j)
    keep_iterate = pltpu.make_async_copy(iterate, iterate_hbm, load_sem.at[7])
    keep_iterate.start()
    link_run(2 * steps - 2)
    link_run(2 * steps - 1)

    sums[0] = jnp.zeros(sums.shape[1:], f32)

    def third(shift):
        def body(i):
            residual = rhs[i] - row_product(i, fine_cols, i, base, blocks, diag, ext2, margin + i)
            sums[i + shift] = residual + sums[chain[i]]

        return body

    for j in reversed(range(steps - early, steps)):
        wait_halo(ext2, 1, j)
        place(ext2, landing2, j)
    for j in range(steps):
        if j < steps - early:
            wait_halo(ext2, 1, j)
            place(ext2, landing2, j)
        for n, start in enumerate((margin - (j + 1) * chunk, margin + j * chunk)):
            rows(start, chunk, third(1 + (2 * j + n) * chunk - start), 2)
        if j < 6:
            rows(cheight // 4 + j * (cheight // 8), cheight // 8, link_coarse, 1)

    def gather(c):
        partial[c] = sums[chain[height + c]]

    rows(0, cheight, gather, 4)

    def slice_of(group, p):
        return pl.ds(piece_of(group, r) * piece + p * share, share)

    def to_partner(o, p):
        src = partial.at[slice_of(((chip + o) % chips) * 2 + 1 - core, p)]
        dst = from_partner.at[o, pl.ds(p * share, share)]
        return remote(src, dst, rs_send.at[o, p], rs_recv.at[o, p], partner)

    order = [*range(1, chips), 0]
    for o in order:
        for p in range(parts):
            to_partner(o, p).start()

    def across(o, p):
        at = pl.ds(p * share, share)
        return remote(chip_send.at[o, at], chip_recv.at[o, at], rc_send.at[o, p], rc_recv.at[o, p], chip_peer(o))

    for o in order:
        start = piece_of(((chip + o) % chips) * 2 + core, r) * piece

        def pack(n):
            chip_send[o, n] = (partial[start + n] + from_partner[o, n]).astype(low)

        def keep(n):
            crhs[n] = partial[start + n] + from_partner[o, n]

        for p in range(parts):
            to_partner(o, p).wait_recv()
            rows(p * share, share, pack if o else keep, 2)
            if o:
                across(o, p).start()
    for c in later_loads[2:]:
        c.wait()

    def coarse_first(n):
        total = crhs[n]
        for o in range(1, chips):
            total = total + chip_recv[o, n].astype(f32)
        crhs[n] = total
        value = damping * dot(csmoother[n], total.astype(low))
        cfirst[n] = value
        cext[reach * piece + n] = value.astype(low)

    def to_shift(d, p):
        at = shifts.index(d)
        return remote(
            cext.at[pl.ds(reach * piece + p * share, share)], cext.at[pl.ds((reach - d) * piece + p * share, share)],
            piece_send.at[at, p], piece_recv.at[at, p], holder(linear + d),
        )

    def each_part(method, d):
        for p in range(parts):
            getattr(to_shift(d, p), method)()

    for p in range(parts):
        for o in range(1, chips):
            across(o, p).wait_recv()
        rows(p * share, share, coarse_first, 2)
        for d in reversed(shifts):
            pl.when(exists(linear + d))(functools.partial(lambda d: to_shift(d, p).start(), d))
    for d in reversed(shifts):
        pl.when(exists(linear - d))(functools.partial(each_part, "wait_recv", d))

    cbase = (linear - reach) * piece

    def coarse_second(n):
        image = row_product(n, coarse_cols, q * piece + n, cbase, cblocks, cdiag, cext, reach * piece + n)
        value = cfirst[n] + damping * dot(csmoother[n], (crhs[n] - image).astype(low))
        correction[q * piece + n] = value.astype(low)

    def piece_to(o, p):
        at = slice_of(g, p)
        return remote(correction.at[at], correction.at[at], ag_send.at[o, p], ag_recv.at[o, p], chip_peer(o))

    def forward(o, p):
        at = slice_of(((chip + o) % chips) * 2 + core, p)
        return remote(correction.at[at], correction.at[at], fwd_send.at[o, p], fwd_recv.at[o, p], partner)

    def put(o, own, p):
        at = slice_of(((chip + o) % chips) * 2 + (core if own else 1 - core), p)
        return pltpu.make_async_copy(correction.at[at], correction_hbm.at[at], out_sem.at[o, own, p])

    for p in range(parts):
        rows(p * share, share, coarse_second, 2)
        for o in range(1, chips):
            piece_to(o, p).start()
        forward(0, p).start()
        put(0, 1, p).start()
    for o in range(1, chips):
        for p in range(parts):
            piece_to(o, p).wait_recv()
            forward(chips - o, p).start()
            put(chips - o, 1, p).start()
    for o in [0, *reversed(range(1, chips))]:
        for p in range(parts):
            forward(o, p).wait_recv()
            put(o, 0, p).start()

    for j in range(steps):
        wait_sent(ext1, 0, j)
        wait_sent(ext2, 1, j)
    for p in range(parts):
        for o in range(chips):
            to_partner(o, p).wait_send()
            forward(o, p).wait_send()
            put(o, 0, p).wait()
            put(o, 1, p).wait()
        for o in range(1, chips):
            across(o, p).wait_send()
            piece_to(o, p).wait_send()
    for d in shifts:
        pl.when(exists(linear + d))(functools.partial(each_part, "wait_send", d))
    keep_iterate.wait()


def add_kernel(
    cheight, aggregate, iterate_hbm, correction_hbm, out_hbm, iterate, correction, in_sem, correction_sem, out_sem
):
    share = iterate.shape[0] // 4
    cshare = cheight // 4
    start = lax.axis_index("rows") * cheight

    def fetch(j):
        at = pl.ds(j * cshare, cshare)
        return pltpu.make_async_copy(correction_hbm.at[at], correction.at[at], correction_sem.at[j])

    def get(j):
        at = pl.ds(j * share, share)
        return pltpu.make_async_copy(iterate_hbm.at[at], iterate.at[at], in_sem.at[j])

    def put(j):
        at = pl.ds(j * share, share)
        return pltpu.make_async_copy(iterate.at[at], out_hbm.at[at], out_sem.at[j])

    for j in range(4):
        fetch(j).start()
    for j in range(4):
        get(j).start()
    for j in range(4):
        fetch(j).wait()
    for j in range(4):
        get(j).wait()

        def step(n, carry):
            i = j * share + n
            iterate[i] = iterate[i] + correction[aggregate[i] - start].astype(f32)
            return carry

        lax.fori_loop(0, share, step, 0, unroll=4)
        put(j).start()
    for j in range(4):
        put(j).wait()


def on_device(
    groups, ranks,
    rhs, fine_diag, fine_smoother, fine_blocks, fine_cols, aggregate,
    coarse_diag, coarse_smoother, coarse_blocks, coarse_cols,
):
    height, b, n = rhs.shape
    cheight = coarse_diag.shape[0]
    neighbours = fine_blocks.shape[1]
    piece = cheight // groups
    chips = groups // 2
    reach = groups // 2
    vmem = pltpu.VMEM
    dma = pltpu.SemaphoreType.DMA
    smem = pl.BlockSpec(memory_space=pltpu.SMEM)
    hbm = pl.BlockSpec(memory_space=pl.ANY)
    iterate, correction = pl.pallas_call(
        functools.partial(kernel, groups, ranks),
        out_shape=(jax.ShapeDtypeStruct(rhs.shape, f32), jax.ShapeDtypeStruct((cheight, b, n), low)),
        in_specs=[smem] * 3 + [hbm] * 7,
        out_specs=(hbm, hbm),
        scratch_shapes=[
            vmem((height, b, n), f32),
            vmem((height, b, b), low),
            vmem((height, b, b), low),
            vmem((height, neighbours, b, b), low),
            vmem((piece, b, b), low),
            vmem((piece, b, b), low),
            vmem((piece, neighbours, b, b), low),
            vmem((2 * height, b, n), low),
            vmem((2 * height, b, n), low),
            vmem((2, height // 2, b, n), low),
            vmem((2, height // 2, b, n), low),
            vmem((height, b, n), f32),
            vmem((height + 1, b, n), f32),
            vmem((cheight, b, n), f32),
            vmem((chips, piece, b, n), f32),
            vmem((chips, piece, b, n), low),
            vmem((chips, piece, b, n), low),
            vmem((piece, b, n), f32),
            vmem((piece, b, n), f32),
            vmem(((2 * reach + 1) * piece, b, n), low),
            vmem((cheight, b, n), low),
            pltpu.SMEM((height + cheight,), jnp.int32),
            dma((8,)),
            dma((chips, 2, parts)),
            dma((2, 2, steps)),
            dma((2, 2, steps)),
            dma((chips, parts)),
            dma((chips, parts)),
            dma((chips, parts)),
            dma((chips, parts)),
            dma((2 * reach, parts)),
            dma((2 * reach, parts)),
            dma((chips, parts)),
            dma((chips, parts)),
            dma((chips, parts)),
            dma((chips, parts)),
        ],
        compiler_params=pltpu.CompilerParams(
            collective_id=0, has_side_effects=True, vmem_limit_bytes=60 * 1024 * 1024
        ),
        name="cycle",
    )(
        fine_cols.T, coarse_cols.T, aggregate,
        rhs, fine_diag, fine_smoother, fine_blocks, coarse_diag, coarse_smoother, coarse_blocks,
    )
    return pl.pallas_call(
        functools.partial(add_kernel, cheight),
        out_shape=jax.ShapeDtypeStruct(rhs.shape, f32),
        in_specs=[smem, hbm, hbm],
        out_specs=hbm,
        scratch_shapes=[vmem((height, b, n), f32), vmem((cheight, b, n), low), dma((4,)), dma((4,)), dma((4,))],
        name="add",
    )(aggregate, iterate, correction)


def solution(mesh):
    fine = P(("grp", "rows"))
    return jax.shard_map(
        functools.partial(on_device, mesh.shape["grp"], mesh.shape["rows"]),
        mesh=mesh,
        in_specs=(fine,) * 6 + (P("rows"),) * 4,
        out_specs=fine,
        check_vma=False,
    )
```
